32 devices in a mesh: node: 8 (over y, x, core), stripe: 4 (over z).
Axes of the slice: x: 2, y: 2, z: 4, core: 2. Of those that a mesh axis runs over, the one named last changes fastest.
Arguments:
- groups: bfloat16 [4, 16, 256, 8, 512], P('stripe', 'node'), may hold values from -21 to 21
- gamma: float32 [8, 8], replicated, may hold values from -2 to 2
- coeffs: float32 [4, 12, 8, 8], replicated, may hold values from -0.625 to 0.625
Outputs:
- syndrome: float32 [256, 4, 4, 8, 512], P('node', 'stripe')
- scores: float32 [256, 4, 4], P('node', 'stripe')
The draws below stay inside these ranges and needn't reach their ends.
All inputs are finite; a program needn't handle non-finite values.
Results may differ from the reference program's by a relative error of at most 0.0003.
Values may be sent and summed in bfloat16 or wider, within the bound.
No kernel may reach another device: no remote copies, remote signals or barrier semaphores. Data moves between devices by JAX's collectives and lax.ppermute only.
A program may use at most 64 MiB of HBM per device.

```python
import jax
import jax.numpy as jnp
from jax import lax

NODES = 16
LAYERS = 256
PLANES = 8
PARITY = 4
DATA_NODES = 12
VIRTUAL = 2
BYTES = 512
STRIPES = 4


def draw_groups(key, part):
    array_shape = (STRIPES, NODES, LAYERS, PLANES, BYTES)
    key_main = jax.random.fold_in(key, 0)
    position = jnp.arange(STRIPES, dtype=jnp.float32) / max(STRIPES - 1, 1)
    stripe_scale = 0.3 * 10.0 ** position
    values = jnp.clip(jax.random.normal(key_main, array_shape), -4.0, 4.0)
    values = values * stripe_scale[:, None, None, None, None]
    return values.astype(jnp.bfloat16)


def noise(own_key, dims, spread, reach, kind=jnp.bfloat16):
    result = spread * jax.random.normal(own_key, dims, jnp.float32)
    return jnp.clip(result, min=-reach, max=reach).astype(kind)


def setup_inputs(seed: int = 0) -> dict:
    seeds = jax.random.split(jax.random.key(seed), 4)
    groups = draw_groups(jax.random.fold_in(seeds[3], 71), 0)
    gamma = noise(seeds[1], (PLANES, PLANES), PLANES ** -0.5, 2.0, jnp.float32)
    coeffs = noise(seeds[2], (PARITY, DATA_NODES, PLANES, PLANES), (DATA_NODES * PLANES) ** -0.5, 0.625, jnp.float32)
    return dict(groups=groups, gamma=gamma, coeffs=coeffs)


precise = lax.Precision.HIGHEST
epsilon = 1e-06

def mix_planes(matrix, values):
    return jnp.einsum('pq,...qb->...pb', matrix, values, precision=precise)

def inverse_factor(gamma):
    order_count = gamma.shape[0]
    identity = jnp.eye(order_count, dtype=jnp.float32)
    mixed = identity + jnp.dot(gamma.T, gamma, precision=precise)
    factor = jnp.linalg.cholesky(mixed)
    solved_rows = []
    for row_at in range(order_count):
        running = identity[row_at]
        for earlier in range(row_at):
            running = running - factor[row_at, earlier] * solved_rows[earlier]
        solved_rows.append(running / factor[row_at, row_at])
    solved = jnp.stack(solved_rows)
    return jnp.dot(solved.T, solved, precision=precise)

def uncouple(stripe_group, gamma, inverse):
    node_grid = stripe_group.reshape(4, 4, 4, 4, 4, 4, PLANES, BYTES)
    outputs = []
    for row_at in range(4):
        row_nodes = node_grid[:, row_at]
        digit_axis = 4 - row_at
        partner_rows = jnp.swapaxes(row_nodes, 0, digit_axis)
        column_ids = jnp.arange(4).reshape(4, 1, 1, 1, 1, 1, 1)
        axis_shape = [1, 1, 1, 1, 1, 1, 1]
        axis_shape[digit_axis] = 4
        digit_ids = jnp.arange(4).reshape(axis_shape)
        own_lower = column_ids < digit_ids
        lower_rows = jnp.where(own_lower, row_nodes, partner_rows)
        upper_rows = jnp.where(own_lower, partner_rows, row_nodes)
        upper_part = mix_planes(inverse, upper_rows + mix_planes(gamma.T, lower_rows))
        uncoupled = jnp.where(own_lower, lower_rows - mix_planes(gamma, upper_part), upper_part)
        uncoupled = jnp.where(column_ids == digit_ids, row_nodes, uncoupled)
        outputs.append(uncoupled)
    return jnp.stack(outputs, axis=1).reshape(NODES, LAYERS, PLANES, BYTES)

def reference(groups, gamma, coeffs):
    inverse = inverse_factor(gamma)
    node_ids = jnp.arange(NODES)
    keep_mask = ((node_ids < DATA_NODES - VIRTUAL) | (node_ids >= DATA_NODES)).astype(jnp.float32)

    def per_stripe(stripe_group):
        values = stripe_group.astype(jnp.float32) * keep_mask[:, None, None, None]
        uncoupled = uncouple(values, gamma, inverse)
        encoded = jnp.einsum('ijpq,jlqb->ilpb', coeffs, uncoupled[:DATA_NODES], precision=precise)
        return uncoupled[DATA_NODES:] - encoded
    syndrome = lax.map(per_stripe, groups)
    syndrome = jnp.transpose(syndrome, (2, 0, 1, 3, 4))
    energy = jnp.mean(syndrome * syndrome, axis=(3, 4))
    pool_mean = jnp.sum(energy, axis=1, keepdims=True) / STRIPES + epsilon
    return (syndrome, energy / pool_mean)
```

```python
import jax
import jax.numpy as jnp
from jax import lax
from jax.experimental import pallas as pl
from jax.experimental.pallas import tpu as pltpu
from jax.sharding import PartitionSpec as P

PLANES = 8
PARITY = 4
DATA_NODES = 12
VIRTUAL = 2
OUT_ROWS = PARITY * PLANES
PARTS = 3


precise = lax.Precision.HIGHEST
epsilon = 1e-06
MIB = 1024 * 1024


def dot32(a, b):
    return jnp.dot(a, b, precision=precise)


def inverse_factor(gamma):
    order_count = gamma.shape[0]
    identity = jnp.eye(order_count, dtype=jnp.float32)
    mixed = identity + dot32(gamma.T, gamma)
    factor = jnp.linalg.cholesky(mixed)
    solved_rows = []
    for row_at in range(order_count):
        running = identity[row_at]
        for earlier in range(row_at):
            running = running - factor[row_at, earlier] * solved_rows[earlier]
        solved_rows.append(running / factor[row_at, row_at])
    solved = jnp.stack(solved_rows)
    return dot32(solved.T, solved)


def split_parts(matrix):
    parts = []
    rest = matrix
    for _ in range(PARTS):
        head = lax.reduce_precision(rest, 8, 7)
        parts.append(head.astype(jnp.bfloat16))
        rest = rest - head
    return jnp.concatenate(parts, axis=-1)


def build_tables(gamma, coeffs, column, first_row, nodes_here):
    inverse = inverse_factor(gamma)
    identity = jnp.eye(PLANES, dtype=jnp.float32)
    rows = first_row + jnp.arange(nodes_here)
    by_column = coeffs.reshape(PARITY, 3, 4, PLANES, PLANES)
    here = lax.dynamic_slice_in_dim(by_column, first_row, nodes_here, axis=2)
    data_part = -jnp.transpose(here, (1, 2, 0, 3, 4))
    own_parity = (jnp.arange(PARITY)[None, :] == rows[:, None]).astype(jnp.float32)
    parity_part = own_parity[None, :, :, None, None] * identity
    plain = jnp.concatenate([data_part, parity_part], axis=0)
    plain = plain.reshape(4, nodes_here, OUT_ROWS, PLANES)
    gain = dot32(gamma, inverse)
    lower = dot32(plain, identity - dot32(gain, gamma.T))
    upper = dot32(plain, inverse)
    from_upper = -dot32(plain, gain)
    from_lower = dot32(plain, dot32(inverse, gamma.T))

    ids = jnp.arange(4)
    offsets = column ^ ids
    pick = (offsets[:, None] == ids[None, :]).astype(jnp.float32)

    def at_offsets(table):
        return jnp.sum(pick[:, :, None, None, None] * table[None], axis=1)

    plain_o, lower_o, upper_o = at_offsets(plain), at_offsets(lower), at_offsets(upper)
    last = (rows == 3)[:, None, None]
    digit = jnp.where(last, column, ids[None, None, :])
    source = offsets[None, :, None]
    real = 4 * offsets[None, :] + rows[:, None]
    real = ((real < DATA_NODES - VIRTUAL) | (real >= DATA_NODES)).astype(jnp.float32)

    def expand(condition):
        return condition[:, :, :, None, None]

    def rows_first(table):
        return jnp.swapaxes(table, 0, 1)[:, :, None]

    own_term = jnp.where(
        expand(source == digit),
        rows_first(plain_o),
        jnp.where(expand(source < digit), rows_first(lower_o), rows_first(upper_o)),
    )
    other = jnp.where(
        (ids[None, :] < offsets[:, None])[:, :, None, None, None], from_upper[None], from_lower[None]
    )
    other = jnp.where((ids[None, :] != offsets[:, None])[:, :, None, None, None], other, 0.0)
    blocks = []
    for at in range(4):
        same = (ids == at)[None, None, :]
        hit = (source == ids[None, None, :]) & ~last
        blocks.append(
            jnp.where(expand(same & (last | ~last)), own_term, 0.0)
            + jnp.where(expand(hit), jnp.swapaxes(other[:, at], 0, 1)[:, :, None], 0.0)
        )
    lines = jnp.concatenate(blocks, axis=-1) * real[:, :, None, None, None]
    away = jnp.where(
        (offsets < column)[:, None, None],
        at_offsets(from_upper)[:, -1],
        at_offsets(from_lower)[:, -1],
    )
    keep = (rows[-1] == 3).astype(jnp.float32) * real[-1, 0]
    away = jnp.where((ids > 0)[:, None, None], away, 0.0) * keep
    extra = jnp.concatenate([away[at] for at in range(4)], axis=-1)
    return split_parts(lines), split_parts(extra)


def gathered(slabs):
    block = jnp.concatenate([slab.astype(jnp.float32) for slab in slabs], axis=0)
    block = block.astype(jnp.bfloat16)
    return jnp.concatenate([block] * PARTS, axis=0)


def line_of(layer, row):
    shift = 2 * jnp.minimum(row, 2)
    digit = (layer >> shift) & 3
    base = layer - (digit << shift)
    return digit, [base + (at << shift) for at in range(4)]


def near_kernel(layers_here, place_ref, own_ref, *refs):
    near_refs, (lines_ref, extra_ref, out_ref) = refs[:-3], refs[-3:]
    nodes_here = own_ref.shape[1]
    column_layers, _, byte_count = out_ref.shape
    column, peer = place_ref[0], place_ref[1]
    first_row = peer * nodes_here

    def body(at, carry):
        layer = at ^ (peer * layers_here)
        total = jnp.zeros((OUT_ROWS, byte_count), jnp.float32)
        for local in range(nodes_here):
            digit, line = line_of(layer, first_row + local)
            own = gathered([own_ref[0, local, column * column_layers + place] for place in line])
            total += jnp.dot(lines_ref[local, 0, digit], own, preferred_element_type=jnp.float32)
            for offset, ref in enumerate(near_refs, start=1):
                block = gathered([ref[0, local, place] for place in line])
                total += jnp.dot(
                    lines_ref[local, offset, digit], block, preferred_element_type=jnp.float32
                )
        away = gathered(
            [own_ref[0, nodes_here - 1, (column ^ o) * column_layers + layer] for o in range(4)]
        )
        total += jnp.dot(extra_ref[...], away, preferred_element_type=jnp.float32)
        out_ref[at] = total
        return carry

    lax.fori_loop(0, column_layers, body, 0, unroll=2)


def far_kernel(layers_here, slot, place_ref, far_ref, lines_ref, near_ref, out_ref):
    nodes_here = far_ref.shape[1]
    peer = place_ref[1]
    first_row = peer * nodes_here

    def body(at, carry):
        layer = (slot * layers_here + at) ^ (peer * layers_here)
        total = near_ref[at]
        for local in range(nodes_here):
            digit, line = line_of(layer, first_row + local)
            block = gathered([far_ref[0, local, place] for place in line])
            total += jnp.dot(lines_ref[local, digit], block, preferred_element_type=jnp.float32)
        out_ref[at] = total
        return carry

    lax.fori_loop(0, layers_here, body, 0, unroll=4)


def finish_kernel(*refs):
    parts, (out_ref, energy_ref) = refs[:-2], refs[-2:]
    layers_here, _, byte_count = out_ref.shape
    rows = []
    for at in range(layers_here):
        value = parts[0][at]
        for part in parts[1:]:
            value = value + part[at]
        out_ref[at] = value
        square = (value * value).reshape(PARITY, PLANES, byte_count)
        lanes = jnp.sum(square, axis=1)
        rows.append(sum(lanes[:, i * 128 : (i + 1) * 128] for i in range(byte_count // 128)))
    stacked = jnp.concatenate(rows, axis=0)
    energy_ref[...] = jnp.sum(stacked.T, axis=0, keepdims=True)


def whole(shape):
    return pl.BlockSpec(shape, lambda: (0,) * len(shape), memory_space=pltpu.VMEM)


def local(groups, gamma, coeffs):
    stripes_here, nodes_here, layers, planes, byte_count = groups.shape
    devices = lax.axis_size("node")
    peers = devices // 4
    layers_here = layers // devices
    column_layers = layers // 4
    device = lax.axis_index("node")
    column, peer = device // peers, device % peers
    place = jnp.stack([column, peer]).astype(jnp.int32)

    received = []
    for offset in range(1, 4):
        piece = lax.dynamic_slice_in_dim(
            groups, (column ^ offset) * column_layers, column_layers, axis=2
        )
        route = [(i, ((i // peers) ^ offset) * peers + i % peers) for i in range(devices)]
        received.append(lax.ppermute(piece, "node", route))
    lines, extra = build_tables(gamma, coeffs, column, peer * nodes_here, nodes_here)

    smem = pl.BlockSpec(memory_space=pltpu.SMEM)
    vmem = pl.BlockSpec(memory_space=pltpu.VMEM)
    sums = jax.ShapeDtypeStruct((column_layers, OUT_ROWS, byte_count), jnp.float32)
    near = pl.pallas_call(
        lambda *refs: near_kernel(layers_here, *refs),
        out_shape=sums,
        in_specs=[smem, vmem, vmem, vmem, vmem, vmem],
        out_specs=vmem,
        compiler_params=pltpu.CompilerParams(vmem_limit_bytes=24 * MIB),
        name="near",
        cost_estimate=pl.CostEstimate(
            flops=4_000_000_000, bytes_accessed=12 * MIB, transcendentals=0
        ),
    )(place, groups, received[0], received[1], lines, extra)

    part = jax.ShapeDtypeStruct((layers_here, OUT_ROWS, byte_count), jnp.float32)
    far_lines = lines[:, 3]

    def far(slot):
        return pl.pallas_call(
            lambda *refs: far_kernel(layers_here, slot, *refs),
            out_shape=part,
            grid=(1,),
            in_specs=[
                smem,
                pl.BlockSpec(received[2].shape, lambda i: (0,) * 5),
                pl.BlockSpec(far_lines.shape, lambda i: (0,) * 4),
                pl.BlockSpec(part.shape, lambda i: (slot, 0, 0)),
            ],
            out_specs=pl.BlockSpec(part.shape, lambda i: (0, 0, 0)),
            compiler_params=pltpu.CompilerParams(vmem_limit_bytes=24 * MIB),
            name="far",
            cost_estimate=pl.CostEstimate(
                flops=1_000_000_000, bytes_accessed=5 * MIB, transcendentals=0
            ),
        )(place, received[2], far_lines, near)

    parts = []
    for slot in range(1, peers):
        route = [(i, (i // peers) * peers + ((i % peers) ^ slot)) for i in range(devices)]
        parts.append(lax.ppermute(far(slot), "node", route))
    parts.append(far(0))
    syndrome, energy = pl.pallas_call(
        finish_kernel,
        out_shape=(part, jax.ShapeDtypeStruct((1, layers_here * PARITY), jnp.float32)),
        in_specs=[vmem] * peers,
        out_specs=(vmem, vmem),
        compiler_params=pltpu.CompilerParams(vmem_limit_bytes=24 * MIB),
        name="finish",
    )(*parts)
    energy = energy / (planes * byte_count)
    stripes = lax.axis_size("stripe")
    pool = energy
    if stripes <= 4:
        for step in range(1, stripes):
            pool = pool + lax.ppermute(
                energy, "stripe", [(i, (i + step) % stripes) for i in range(stripes)]
            )
    else:
        pool = lax.psum(energy, "stripe")
    scores = energy / (pool / (stripes * stripes_here) + epsilon)
    return (
        syndrome.reshape(layers_here, stripes_here, PARITY, planes, byte_count),
        scores.reshape(layers_here, stripes_here, PARITY),
    )


def solution(mesh):
    return jax.shard_map(
        local,
        mesh=mesh,
        in_specs=(P("stripe", "node", None, None, None), P(), P()),
        out_specs=(P("node", "stripe", None, None, None), P("node", "stripe", None)),
        check_vma=False,
    )
```

```python
import jax
import jax.numpy as jnp
from jax import lax
from jax.experimental import pallas as pl
from jax.experimental.pallas import tpu as pltpu
from jax.sharding import PartitionSpec as P


PLANES = 8
PARITY = 4
DATA_NODES = 12
VIRTUAL = 2
OUT_ROWS = PARITY * PLANES
PARTS = 3


precise = lax.Precision.HIGHEST
epsilon = 1e-06
WIDTH = PARTS * 4 * PLANES
MIB = 1024 * 1024


def dot32(a, b):
    return jnp.dot(a, b, precision=precise)


def inverse_of(matrix):
    size = matrix.shape[0]
    row_ids = lax.broadcasted_iota(jnp.int32, (size, size), 0)
    left = matrix
    right = (row_ids == lax.broadcasted_iota(jnp.int32, (size, size), 1)).astype(jnp.float32)
    for at in range(size):
        scale = 1.0 / left[at : at + 1, at : at + 1]
        left_row = left[at : at + 1] * scale
        right_row = right[at : at + 1] * scale
        factor = left[:, at : at + 1]
        here = row_ids == at
        left = jnp.where(here, left_row, left - factor * left_row)
        right = jnp.where(here, right_row, right - factor * right_row)
    return 0.5 * (right + right.T)


def table_kernel(place_ref, gamma_ref, gamma_t_ref, encode_ref, lines_ref, extra_ref):
    column = place_ref[0]
    gamma, gamma_t = gamma_ref[...], gamma_t_ref[...]
    eye_rows = lax.broadcasted_iota(jnp.int32, (PLANES, PLANES), 0)
    eye_lanes = lax.broadcasted_iota(jnp.int32, (PLANES, PLANES), 1)
    identity = (eye_rows == eye_lanes).astype(jnp.float32)
    inverse = inverse_of(identity + dot32(gamma_t, gamma))
    gain = dot32(gamma, inverse)
    wide_rows = lax.broadcasted_iota(jnp.int32, (PLANES, WIDTH), 0)
    wide_lanes = lax.broadcasted_iota(jnp.int32, (PLANES, WIDTH), 1)
    spread = (wide_rows == wide_lanes % PLANES).astype(jnp.float32)

    def tiled(matrix):
        return jnp.concatenate([dot32(matrix, spread)] * 4, axis=0)

    plain = jnp.concatenate([spread] * 4, axis=0)
    lower = tiled(identity - dot32(gain, gamma_t))
    upper = tiled(inverse)
    from_upper = tiled(-gain)
    from_lower = tiled(dot32(inverse, gamma_t))
    block_in = lax.broadcasted_iota(jnp.int32, (4 * PLANES, WIDTH), 0) // PLANES
    lanes = lax.broadcasted_iota(jnp.int32, (4 * PLANES, WIDTH), 1)
    block_out = (lanes // PLANES) % 4
    zero = jnp.zeros((4 * PLANES, WIDTH), jnp.float32)

    def parts(product):
        part = lax.broadcasted_iota(jnp.int32, product.shape, 1) // (4 * PLANES)
        head = product.astype(jnp.bfloat16).astype(jnp.float32)
        rest = product - head
        middle = rest.astype(jnp.bfloat16).astype(jnp.float32)
        tail = rest - middle
        chosen = jnp.where(part == 0, head, jnp.where(part == 1, middle, tail))
        return chosen.astype(jnp.bfloat16)

    def real(source, row):
        node = 4 * source + row
        return jnp.where((node < DATA_NODES - VIRTUAL) | (node >= DATA_NODES), 1.0, 0.0)

    upto3 = jnp.concatenate([encode_ref[row] for row in range(3)], axis=0)
    for o in range(4):
        source = column ^ o

        def own(digit):
            return jnp.where(source == digit, plain, jnp.where(source < digit, lower, upper))

        coupled = jnp.where(block_out < source, from_upper, from_lower)
        coupled = jnp.where((block_in == block_out) & (block_in != source), coupled, zero)
        for j in range(4):
            from_own = (block_in == source) & (block_out == j)
            step = jnp.where(from_own, own(j), jnp.where(source == j, coupled, zero))
            product = dot32(upto3, step)
            for row in range(3):
                piece = product[row * OUT_ROWS : (row + 1) * OUT_ROWS] * real(source, row)
                lines_ref[row, o, j * OUT_ROWS : (j + 1) * OUT_ROWS] = parts(piece)
            piece = dot32(encode_ref[3], jnp.where(from_own, own(column), zero))
            piece = piece * real(source, 3)
            lines_ref[3, o, j * OUT_ROWS : (j + 1) * OUT_ROWS] = parts(piece)
    away = jnp.where(block_in < column, from_upper, from_lower)
    away = jnp.where((block_in == (column ^ block_out)) & (block_out != 0), away, zero)
    extra_ref[...] = parts(dot32(encode_ref[3], away) * real(column, 3))


def build_tables(place, gamma, coeffs):
    by_column = coeffs.reshape(PARITY, 3, 4, PLANES, PLANES)
    data_part = -jnp.transpose(by_column, (2, 0, 3, 1, 4)).reshape(4, OUT_ROWS, 3 * PLANES)
    own_parity = jnp.arange(OUT_ROWS)[None, :] - PLANES * jnp.arange(4)[:, None]
    parity_part = (own_parity[:, :, None] == jnp.arange(PLANES)).astype(jnp.float32)
    encode = jnp.concatenate([data_part, parity_part], axis=-1)
    vmem = pl.BlockSpec(memory_space=pltpu.VMEM)
    return pl.pallas_call(
        table_kernel,
        out_shape=(
            jax.ShapeDtypeStruct((4, 4, 4 * OUT_ROWS, WIDTH), jnp.bfloat16),
            jax.ShapeDtypeStruct((OUT_ROWS, WIDTH), jnp.bfloat16),
        ),
        in_specs=[pl.BlockSpec(memory_space=pltpu.SMEM), vmem, vmem, vmem],
        out_specs=(vmem, vmem),
        compiler_params=pltpu.CompilerParams(vmem_limit_bytes=16 * MIB),
        name="tables",
        cost_estimate=pl.CostEstimate(flops=1_000_000_000, bytes_accessed=MIB, transcendentals=0),
    )(place, gamma, gamma.T, encode)


def gathered(slabs):
    block = jnp.concatenate([slab.astype(jnp.float32) for slab in slabs], axis=0)
    block = block.astype(jnp.bfloat16)
    return jnp.concatenate([block] * PARTS, axis=0)


def line_at(number, row):
    shift = 2 * jnp.minimum(row, 2)
    base = ((number >> shift) << (shift + 2)) | (number & ((1 << shift) - 1))
    return [base + (at << shift) for at in range(4)]


def mixed(matrix, slabs):
    return jnp.dot(matrix, gathered(slabs), preferred_element_type=jnp.float32)


def own_kernel(layers_here, place_ref, own_ref, lines_ref, extra_ref, out_ref):
    nodes_here = own_ref.shape[1]
    column_layers = out_ref.shape[0]
    column, peer = place_ref[0], place_ref[1]
    flip = peer * layers_here
    for local in range(nodes_here):
        row = peer * nodes_here + local

        def body(number, carry):
            line = line_at(number, row)
            total = mixed(
                lines_ref[row, 0],
                [own_ref[0, local, column * column_layers + layer] for layer in line],
            )
            for at, layer in enumerate(line):
                value = total[at * OUT_ROWS : (at + 1) * OUT_ROWS]
                spot = layer ^ flip
                out_ref[spot] = value if local == 0 else out_ref[spot] + value
            return carry

        lax.fori_loop(0, column_layers // 4, body, 0, unroll=2)

    @pl.when((peer + 1) * nodes_here == 4)
    def _():
        def body(layer, carry):
            away = [
                own_ref[0, nodes_here - 1, (column ^ o) * column_layers + layer] for o in range(4)
            ]
            out_ref[layer ^ flip] += mixed(extra_ref[...], away)
            return carry

        lax.fori_loop(0, column_layers, body, 0, unroll=4)


def add_rows(layers_here, nodes_here, place_ref, lines_ref, pieces, before_ref, total_ref):
    peer = place_ref[1]
    flip = peer * layers_here
    for order, (local, sources) in enumerate(pieces.items()):
        row = peer * nodes_here + local

        def body(number, carry):
            line = line_at(number, row)
            total = None
            for offset, ref in sources:
                term = mixed(lines_ref[row, offset], [ref[0, 0, layer] for layer in line])
                total = term if total is None else total + term
            for at, layer in enumerate(line):
                spot = layer ^ flip
                start = before_ref[spot] if order == 0 else total_ref[spot]
                total_ref[spot] = start + total[at * OUT_ROWS : (at + 1) * OUT_ROWS]
            return carry

        lax.fori_loop(0, total_ref.shape[0] // 4, body, 0, unroll=2)


def across_kernel(layers_here, nodes_here, place_ref, lines_ref, before_ref, far_ref, total_ref):
    pieces = {at: [(3, far_ref.at[:, pl.ds(at, 1)])] for at in range(nodes_here)}
    add_rows(layers_here, nodes_here, place_ref, lines_ref, pieces, before_ref, total_ref)


def beside_kernel(layers_here, nodes_here, rows, place_ref, lines_ref, before_ref, *refs):
    piece_refs, out_refs, total_ref = refs[: 2 * rows], refs[2 * rows : -1], refs[-1]
    pieces = {at: [(1, piece_refs[2 * at]), (2, piece_refs[2 * at + 1])] for at in range(rows)}
    add_rows(layers_here, nodes_here, place_ref, lines_ref, pieces, before_ref, total_ref)
    for slot in reversed(range(len(out_refs))):

        def copy(at, carry):
            out_refs[slot][at] = total_ref[slot * layers_here + at]
            return carry

        lax.fori_loop(0, layers_here, copy, 0, unroll=4)


def finish_kernel(nodes_here, place_ref, lines_ref, before_ref, *refs):
    piece_refs, refs = refs[:-5], refs[-5:]
    out_ref, energy_ref, value_ref, lanes_ref, sems = refs
    layers_here, _, byte_count = value_ref.shape
    peer = place_ref[1]
    copies = []
    for first in range(0, layers_here, 16):
        for number in range(4):
            line = [first + number + 4 * at for at in range(4)]
            total = None
            for order, ref in enumerate(piece_refs):
                row = (peer ^ (order // 2)) * nodes_here + nodes_here - 1
                term = mixed(lines_ref[row, 1 + order % 2], [ref[0, 0, layer] for layer in line])
                total = term if total is None else total + term
            for at, layer in enumerate(line):
                value = before_ref[layer]
                if total is not None:
                    value = value + total[at * OUT_ROWS : (at + 1) * OUT_ROWS]
                value_ref[layer] = value
                square = value * value
                lanes = sum(square[:, i * 128 : (i + 1) * 128] for i in range(byte_count // 128))
                for i in range(PARITY):
                    lanes_ref[i, layer : layer + 1] = jnp.sum(
                        lanes[i * PLANES : (i + 1) * PLANES], axis=0, keepdims=True
                    )
        rows = pl.ds(first, 16)
        copy = pltpu.make_async_copy(value_ref.at[rows], out_ref.at[rows], sems.at[first // 16])
        copy.start()
        copies.append(copy)
    sums = [jnp.sum(lanes_ref[i], axis=1, keepdims=True) for i in range(PARITY)]
    energy_ref[...] = jnp.concatenate(sums, axis=1) * (1.0 / (PLANES * byte_count))
    for copy in copies:
        copy.wait()


def kernel_call(body, out_shape, operands, mflops, mib, out_specs=None, scratch=()):
    smem = pl.BlockSpec(memory_space=pltpu.SMEM)
    vmem = pl.BlockSpec(memory_space=pltpu.VMEM)
    if out_specs is None:
        out_specs = jax.tree.map(lambda _: vmem, out_shape)
    return pl.pallas_call(
        body,
        out_shape=out_shape,
        in_specs=[smem] + [vmem] * (len(operands) - 1),
        out_specs=out_specs,
        scratch_shapes=scratch,
        compiler_params=pltpu.CompilerParams(vmem_limit_bytes=24 * MIB),
        cost_estimate=pl.CostEstimate(
            flops=mflops * 1_000_000, bytes_accessed=mib * MIB, transcendentals=0
        ),
    )(*operands)


def scrub(groups, gamma, coeffs):
    stripes_here, nodes_here, layers, planes, byte_count = groups.shape
    devices = lax.axis_size("node")
    peers = devices // 4
    layers_here = layers // devices
    column_layers = layers // 4
    device = lax.axis_index("node")
    column, peer = device // peers, device % peers
    place = jnp.stack([column, peer]).astype(jnp.int32)
    direct = nodes_here == 2
    rows = nodes_here - 1 if direct else nodes_here

    def cut(source, first_row, row_count, offset, slot=None):
        first, count = (column ^ offset) * column_layers, column_layers
        if slot is not None:
            first, count = first + (peer ^ slot) * layers_here, layers_here
        return lax.dynamic_slice(
            source,
            (0, first_row, first, 0, 0),
            (stripes_here, row_count, count, planes, byte_count),
        )

    def send(piece, offset, slot=0):
        route = [(i, (((i // peers) ^ offset) * peers + i % peers) ^ slot) for i in range(devices)]
        return lax.ppermute(piece, "node", route)

    across_piece = cut(groups, 0, nodes_here, 3)
    source, across_piece = lax.optimization_barrier((groups, across_piece))
    across_piece = send(across_piece, 3)
    plan = [(at, 1, offset, None) for at in range(rows) for offset in (1, 2)]
    if direct:
        plan += [(rows, 1, offset, slot) for slot in range(peers) for offset in (1, 2)]
    cuts = [cut(source, *entry) for entry in plan]
    cuts = lax.optimization_barrier(tuple(cuts))
    arrived = [send(piece, entry[2], entry[3] or 0) for piece, entry in zip(cuts, plan)]
    beside_pieces, last_pieces = arrived[: 2 * rows], arrived[2 * rows :]
    lines, extra = build_tables(place, gamma, coeffs)

    all_layers = jax.ShapeDtypeStruct((column_layers, OUT_ROWS, byte_count), jnp.float32)
    part = jax.ShapeDtypeStruct((layers_here, OUT_ROWS, byte_count), jnp.float32)
    own = kernel_call(
        lambda *refs: own_kernel(layers_here, *refs),
        all_layers,
        (place, groups, lines, extra),
        2000,
        8,
    )
    across = kernel_call(
        lambda *refs: across_kernel(layers_here, nodes_here, *refs),
        all_layers,
        (place, lines, own, across_piece),
        2000,
        9,
    )
    sums = kernel_call(
        lambda *refs: beside_kernel(layers_here, nodes_here, rows, *refs),
        [part] * peers,
        (place, lines, across, *beside_pieces),
        2000,
        9,
        scratch=[pltpu.VMEM(all_layers.shape, jnp.float32)],
    )
    total = sums[0]
    for slot in range(1, peers):
        route = [(i, (i // peers) * peers + ((i % peers) ^ slot)) for i in range(devices)]
        total = total + lax.ppermute(sums[slot], "node", route)

    syndrome, energy = kernel_call(
        lambda *refs: finish_kernel(nodes_here, *refs),
        (part, jax.ShapeDtypeStruct((layers_here, PARITY), jnp.float32)),
        (place, lines, total, *last_pieces),
        500,
        4,
        out_specs=(
            pl.BlockSpec(memory_space=pl.ANY),
            pl.BlockSpec(memory_space=pltpu.VMEM),
        ),
        scratch=[
            pltpu.VMEM(part.shape, jnp.float32),
            pltpu.VMEM((PARITY, layers_here, 128), jnp.float32),
            pltpu.SemaphoreType.DMA((layers_here // 16,)),
        ],
    )
    stripes = lax.axis_size("stripe")
    pool = energy
    if stripes & (stripes - 1) == 0:
        distance = 1
        while distance < stripes:
            pool = pool + lax.ppermute(
                pool, "stripe", [(i, i ^ distance) for i in range(stripes)]
            )
            distance *= 2
    else:
        pool = lax.psum(energy, "stripe")
    scores = energy / (pool / (stripes * stripes_here) + epsilon)
    return (
        syndrome.reshape(layers_here, stripes_here, PARITY, planes, byte_count),
        scores.reshape(layers_here, stripes_here, PARITY),
    )


def solution(mesh):
    return jax.shard_map(
        scrub,
        mesh=mesh,
        in_specs=(P("stripe", "node", None, None, None), P(), P()),
        out_specs=(P("node", "stripe", None, None, None), P("node", "stripe", None)),
        check_vma=False,
    )
```

```python
import jax
import jax.numpy as jnp
from jax import lax
from jax.experimental import pallas as pl
from jax.experimental.pallas import tpu as pltpu
from jax.sharding import PartitionSpec as P


PLANES = 8
PARITY = 4
DATA_NODES = 12
VIRTUAL = 2
OUT_ROWS = PARITY * PLANES
PARTS = 3


precise = lax.Precision.HIGHEST
epsilon = 1e-06
WIDTH = PARTS * 4 * PLANES
MIB = 1024 * 1024


def dot32(a, b):
    return jnp.dot(a, b, precision=precise)


def inverse_of(matrix):
    size = matrix.shape[0]
    row_ids = lax.broadcasted_iota(jnp.int32, (size, size), 0)
    left = matrix
    right = (row_ids == lax.broadcasted_iota(jnp.int32, (size, size), 1)).astype(jnp.float32)
    for at in range(size):
        scale = 1.0 / left[at : at + 1, at : at + 1]
        left_row = left[at : at + 1] * scale
        right_row = right[at : at + 1] * scale
        factor = left[:, at : at + 1]
        here = row_ids == at
        left = jnp.where(here, left_row, left - factor * left_row)
        right = jnp.where(here, right_row, right - factor * right_row)
    return 0.5 * (right + right.T)


def table_kernel(nodes_here, gamma_ref, coeffs_ref, lines_ref, extra_ref):
    column, _ = where_am_i(nodes_here)
    gamma = gamma_ref[...]
    gamma_t = gamma.T
    encode = encode_rows(coeffs_ref[...])
    eye_rows = lax.broadcasted_iota(jnp.int32, (PLANES, PLANES), 0)
    eye_lanes = lax.broadcasted_iota(jnp.int32, (PLANES, PLANES), 1)
    identity = (eye_rows == eye_lanes).astype(jnp.float32)
    inverse = inverse_of(identity + dot32(gamma_t, gamma))
    gain = dot32(gamma, inverse)
    wide_rows = lax.broadcasted_iota(jnp.int32, (PLANES, WIDTH), 0)
    wide_lanes = lax.broadcasted_iota(jnp.int32, (PLANES, WIDTH), 1)
    spread = (wide_rows == wide_lanes % PLANES).astype(jnp.float32)

    def tiled(matrix):
        return jnp.concatenate([dot32(matrix, spread)] * 4, axis=0)

    plain = jnp.concatenate([spread] * 4, axis=0)
    lower = tiled(identity - dot32(gain, gamma_t))
    upper = tiled(inverse)
    from_upper = tiled(-gain)
    from_lower = tiled(dot32(inverse, gamma_t))
    block_in = lax.broadcasted_iota(jnp.int32, (4 * PLANES, WIDTH), 0) // PLANES
    lanes = lax.broadcasted_iota(jnp.int32, (4 * PLANES, WIDTH), 1)
    block_out = (lanes // PLANES) % 4
    zero = jnp.zeros((4 * PLANES, WIDTH), jnp.float32)

    def parts(product):
        part = lax.broadcasted_iota(jnp.int32, product.shape, 1) // (4 * PLANES)
        head = product.astype(jnp.bfloat16).astype(jnp.float32)
        rest = product - head
        middle = rest.astype(jnp.bfloat16).astype(jnp.float32)
        tail = rest - middle
        chosen = jnp.where(part == 0, head, jnp.where(part == 1, middle, tail))
        return chosen.astype(jnp.bfloat16)

    def real(source, row):
        node = 4 * source + row
        return jnp.where((node < DATA_NODES - VIRTUAL) | (node >= DATA_NODES), 1.0, 0.0)

    upto3 = jnp.concatenate(encode[:3], axis=0)
    for o in range(4):
        source = column ^ o

        def own(digit):
            return jnp.where(source == digit, plain, jnp.where(source < digit, lower, upper))

        coupled = jnp.where(block_out < source, from_upper, from_lower)
        coupled = jnp.where((block_in == block_out) & (block_in != source), coupled, zero)
        for j in range(4):
            from_own = (block_in == source) & (block_out == j)
            step = jnp.where(from_own, own(j), jnp.where(source == j, coupled, zero))
            product = dot32(upto3, step)
            for row in range(3):
                piece = product[row * OUT_ROWS : (row + 1) * OUT_ROWS] * real(source, row)
                lines_ref[row, o, j * OUT_ROWS : (j + 1) * OUT_ROWS] = parts(piece)
            piece = dot32(encode[3], jnp.where(from_own, own(column), zero))
            piece = piece * real(source, 3)
            lines_ref[3, o, j * OUT_ROWS : (j + 1) * OUT_ROWS] = parts(piece)
    away = jnp.where(block_in < column, from_upper, from_lower)
    away = jnp.where((block_in == (column ^ block_out)) & (block_out != 0), away, zero)
    extra_ref[...] = parts(dot32(encode[3], away) * real(column, 3))


def encode_rows(coeffs):
    nodes = coeffs.shape[-1]
    flat = coeffs.reshape(OUT_ROWS * PLANES, nodes)
    lanes = lax.broadcasted_iota(jnp.int32, (nodes, 4 * OUT_ROWS), 1)
    node = 4 * ((lanes // PLANES) % 4) + lanes // OUT_ROWS
    pick = lax.broadcasted_iota(jnp.int32, (nodes, 4 * OUT_ROWS), 0) == node
    picked = dot32(flat, pick.astype(jnp.float32)).reshape(OUT_ROWS, PLANES, 4 * OUT_ROWS)
    plane = lax.broadcasted_iota(jnp.int32, picked.shape, 1)
    lane = lax.broadcasted_iota(jnp.int32, picked.shape, 2)
    data = jnp.sum(jnp.where(plane == lane % PLANES, picked, 0.0), axis=1)
    out = lax.broadcasted_iota(jnp.int32, (OUT_ROWS, 4 * PLANES), 0)
    into = lax.broadcasted_iota(jnp.int32, (OUT_ROWS, 4 * PLANES), 1)
    rows = []
    for row in range(4):
        parity = (into // PLANES == 3) & (out == row * PLANES + into % PLANES)
        taken = data[:, row * OUT_ROWS : (row + 1) * OUT_ROWS]
        rows.append(jnp.where(parity, 1.0, -taken))
    return rows


def build_tables(nodes_here, gamma, coeffs):
    return kernel_call(
        lambda *refs: table_kernel(nodes_here, *refs),
        (
            jax.ShapeDtypeStruct((4, 4, 4 * OUT_ROWS, WIDTH), jnp.bfloat16),
            jax.ShapeDtypeStruct((OUT_ROWS, WIDTH), jnp.bfloat16),
        ),
        (gamma, jnp.transpose(coeffs, (0, 2, 3, 1))),
        1000,
        1,
    )


def where_am_i(nodes_here):
    peers = 4 // nodes_here
    device = lax.axis_index("node")
    return device // peers, device % peers


def gathered(slabs):
    block = jnp.concatenate(slabs, axis=0)
    return jnp.concatenate([block] * PARTS, axis=0)


def line_at(number, row):
    shift = 2 * jnp.minimum(row, 2)
    base = ((number >> shift) << (shift + 2)) | (number & ((1 << shift) - 1))
    return [base + (at << shift) for at in range(4)]


def mixed(matrix, slabs):
    return jnp.dot(matrix, gathered(slabs), preferred_element_type=jnp.float32)


def own_kernel(layers_here, own_ref, lines_ref, extra_ref, out_ref):
    nodes_here = own_ref.shape[1]
    column_layers = out_ref.shape[0]
    column, peer = where_am_i(nodes_here)
    flip = peer * layers_here
    for local in range(nodes_here):
        row = peer * nodes_here + local

        def body(number, carry):
            line = line_at(number, row)
            total = mixed(
                lines_ref[row, 0],
                [own_ref[0, local, column * column_layers + layer] for layer in line],
            )
            for at, layer in enumerate(line):
                value = total[at * OUT_ROWS : (at + 1) * OUT_ROWS]
                spot = layer ^ flip
                out_ref[spot] = value if local == 0 else out_ref[spot] + value
            return carry

        lax.fori_loop(0, column_layers // 4, body, 0, unroll=8)

    @pl.when((peer + 1) * nodes_here == 4)
    def _():
        def body(layer, carry):
            away = [
                own_ref[0, nodes_here - 1, (column ^ o) * column_layers + layer] for o in range(4)
            ]
            out_ref[layer ^ flip] += mixed(extra_ref[...], away)
            return carry

        lax.fori_loop(0, column_layers, body, 0, unroll=8)


def add_rows(layers_here, nodes_here, lines_ref, pieces, before_ref, total_ref):
    _, peer = where_am_i(nodes_here)
    flip = peer * layers_here
    for order, (local, sources) in enumerate(pieces.items()):
        row = peer * nodes_here + local

        def body(number, carry):
            line = line_at(number, row)
            total = None
            for offset, ref in sources:
                term = mixed(lines_ref[row, offset], [ref[0, 0, layer] for layer in line])
                total = term if total is None else total + term
            for at, layer in enumerate(line):
                spot = layer ^ flip
                start = before_ref[spot] if order == 0 else total_ref[spot]
                total_ref[spot] = start + total[at * OUT_ROWS : (at + 1) * OUT_ROWS]
            return carry

        lax.fori_loop(0, total_ref.shape[0] // 4, body, 0, unroll=8)


def across_kernel(layers_here, nodes_here, lines_ref, before_ref, far_ref, total_ref):
    pieces = {at: [(3, far_ref.at[:, pl.ds(at, 1)])] for at in range(nodes_here)}
    add_rows(layers_here, nodes_here, lines_ref, pieces, before_ref, total_ref)


def beside_kernel(layers_here, nodes_here, rows, lines_ref, before_ref, *refs):
    piece_refs, out_refs, total_ref = refs[: 2 * rows], refs[2 * rows : -1], refs[-1]
    pieces = {at: [(1, piece_refs[2 * at]), (2, piece_refs[2 * at + 1])] for at in range(rows)}
    add_rows(layers_here, nodes_here, lines_ref, pieces, before_ref, total_ref)
    for slot in reversed(range(len(out_refs))):

        def copy(at, carry):
            out_refs[slot][at] = total_ref[slot * layers_here + at]
            return carry

        lax.fori_loop(0, layers_here, copy, 0, unroll=8)


def join_kernel(nodes_here, sums_count, lines_ref, *refs):
    sum_refs, piece_refs, total_ref = refs[:sums_count], refs[sums_count:-1], refs[-1]
    _, peer = where_am_i(nodes_here)
    row = peer * nodes_here + nodes_here - 1

    def body(number, carry):
        line = line_at(number, jnp.int32(1))
        total = None
        for order, ref in enumerate(piece_refs):
            term = mixed(lines_ref[row, 1 + order % 2], [ref[0, 0, layer] for layer in line])
            total = term if total is None else total + term
        for at, layer in enumerate(line):
            value = sum(ref[layer] for ref in sum_refs)
            if total is not None:
                value = value + total[at * OUT_ROWS : (at + 1) * OUT_ROWS]
            total_ref[layer] = value
        return carry

    lax.fori_loop(0, total_ref.shape[0] // 4, body, 0, unroll=8)


def finish_kernel(nodes_here, lines_ref, before_ref, *refs):
    piece_refs, refs = refs[:-5], refs[-5:]
    out_ref, energy_ref, value_ref, lanes_ref, sems = refs
    layers_here, _, byte_count = value_ref.shape
    _, peer = where_am_i(nodes_here)
    copies = []
    for first in range(0, layers_here, 16):
        for number in range(4):
            line = [first + number + 4 * at for at in range(4)]
            total = None
            for order, ref in enumerate(piece_refs):
                row = (peer ^ (1 + order // 2)) * nodes_here + nodes_here - 1
                term = mixed(lines_ref[row, 1 + order % 2], [ref[0, 0, layer] for layer in line])
                total = term if total is None else total + term
            for at, layer in enumerate(line):
                value = before_ref[layer]
                if total is not None:
                    value = value + total[at * OUT_ROWS : (at + 1) * OUT_ROWS]
                value_ref[layer] = value
                square = value * value
                lanes = sum(square[:, i * 128 : (i + 1) * 128] for i in range(byte_count // 128))
                for i in range(PARITY):
                    lanes_ref[i, layer : layer + 1] = jnp.sum(
                        lanes[i * PLANES : (i + 1) * PLANES], axis=0, keepdims=True
                    )
        rows = pl.ds(first, 16)
        copy = pltpu.make_async_copy(value_ref.at[rows], out_ref.at[rows], sems.at[first // 16])
        copy.start()
        copies.append(copy)
    lanes = jnp.concatenate([lanes_ref[i] for i in range(PARITY)], axis=0)
    energy = jnp.sum(lanes.T, axis=0, keepdims=True) * (1.0 / (PLANES * byte_count))
    for i in range(PARITY):
        energy_ref[0, i : i + 1] = energy[:, i * layers_here : (i + 1) * layers_here]
    for copy in copies:
        copy.wait()


def kernel_call(
    body, out_shape, operands, mflops, mib, in_specs=None, out_specs=None, scratch=(), vmem=16
):
    whole = pl.BlockSpec(memory_space=pltpu.VMEM)
    if out_specs is None:
        out_specs = jax.tree.map(lambda _: whole, out_shape)
    return pl.pallas_call(
        body,
        out_shape=out_shape,
        in_specs=in_specs or [whole] * len(operands),
        out_specs=out_specs,
        scratch_shapes=scratch,
        compiler_params=pltpu.CompilerParams(vmem_limit_bytes=vmem * MIB),
        cost_estimate=pl.CostEstimate(
            flops=mflops * 1_000_000, bytes_accessed=mib * MIB, transcendentals=0
        ),
    )(*operands)


def scrub(groups, gamma, coeffs):
    stripes_here, nodes_here, layers, planes, byte_count = groups.shape
    devices = lax.axis_size("node")
    peers = devices // 4
    layers_here = layers // devices
    column_layers = layers // 4
    direct = nodes_here == 2
    rows = nodes_here - 1 if direct else nodes_here

    def cut(source, plan):
        def body(source_ref, *refs):
            column, peer = where_am_i(nodes_here)
            out_refs, sems = refs[:-1], refs[-1]
            copies = []
            for at, (first_row, row_count, offset, slot) in enumerate(plan):
                first, count = (column ^ offset) * column_layers, column_layers
                if slot is not None:
                    first, count = first + (peer ^ slot) * layers_here, layers_here
                piece = source_ref.at[:, pl.ds(first_row, row_count), pl.ds(first, count)]
                copies.append(pltpu.make_async_copy(piece, out_refs[at], sems.at[at]))
                copies[-1].start()
            for copy in copies:
                copy.wait()

        shapes = [
            (stripes_here, count, column_layers if slot is None else layers_here, planes, byte_count)
            for _, count, _, slot in plan
        ]
        return kernel_call(
            body,
            [jax.ShapeDtypeStruct(shape, groups.dtype) for shape in shapes],
            (source,),
            1,
            3,
            in_specs=[pl.BlockSpec(memory_space=pltpu.HBM)],
            scratch=[pltpu.SemaphoreType.DMA((len(plan),))],
            vmem=16,
        )

    def send(piece, offset, slot=0):
        route = [(i, (((i // peers) ^ offset) * peers + i % peers) ^ slot) for i in range(devices)]
        return lax.ppermute(piece, "node", route)

    column = lax.axis_index("node") // peers
    across_piece = lax.dynamic_slice(
        groups,
        (0, 0, (column ^ 3) * column_layers, 0, 0),
        (stripes_here, nodes_here, column_layers, planes, byte_count),
    )
    source, across_piece = lax.optimization_barrier((groups, across_piece))
    across_piece = send(across_piece, 3)
    plan = [(at, 1, offset, None) for at in range(rows) for offset in (1, 2)]
    if direct:
        plan += [(rows, 1, offset, slot) for slot in range(peers) for offset in (1, 2)]
    cuts = cut(source, plan)
    arrived = [send(piece, entry[2], entry[3] or 0) for piece, entry in zip(cuts, plan)]
    beside_pieces, last_pieces = arrived[: 2 * rows], arrived[2 * rows :]
    lines, extra = build_tables(nodes_here, gamma, coeffs)

    all_layers = jax.ShapeDtypeStruct((column_layers, OUT_ROWS, byte_count), jnp.float32)
    part = jax.ShapeDtypeStruct((layers_here, OUT_ROWS, byte_count), jnp.float32)
    own = kernel_call(
        lambda *refs: own_kernel(layers_here, *refs), all_layers, (groups, lines, extra), 2000, 8
    )
    across = kernel_call(
        lambda *refs: across_kernel(layers_here, nodes_here, *refs),
        all_layers,
        (lines, own, across_piece),
        2000,
        9,
    )
    sums = kernel_call(
        lambda *refs: beside_kernel(layers_here, nodes_here, rows, *refs),
        [part] * peers,
        (lines, across, *beside_pieces),
        2000,
        9,
        scratch=[pltpu.VMEM(all_layers.shape, jnp.float32)],
    )
    parts = [sums[0]]
    for slot in range(1, peers):
        route = [(i, (i // peers) * peers + ((i % peers) ^ slot)) for i in range(devices)]
        parts.append(lax.ppermute(sums[slot], "node", route))
    total = kernel_call(
        lambda *refs: join_kernel(nodes_here, peers, *refs),
        part,
        (lines, *parts, *last_pieces[:2]),
        500,
        6,
    )

    syndrome, energy = kernel_call(
        lambda *refs: finish_kernel(nodes_here, *refs),
        (part, jax.ShapeDtypeStruct((stripes_here, PARITY, layers_here), jnp.float32)),
        (lines, total, *last_pieces[2:]),
        500,
        4,
        out_specs=(
            pl.BlockSpec(memory_space=pl.ANY),
            pl.BlockSpec(memory_space=pltpu.VMEM),
        ),
        scratch=[
            pltpu.VMEM(part.shape, jnp.float32),
            pltpu.VMEM((PARITY, layers_here, 128), jnp.float32),
            pltpu.SemaphoreType.DMA((layers_here // 16,)),
        ],
    )
    stripes = lax.axis_size("stripe")
    pool = energy
    if stripes & (stripes - 1) == 0:
        distance = 1
        while distance < stripes:
            pool = pool + lax.ppermute(
                pool, "stripe", [(i, i ^ distance) for i in range(stripes)]
            )
            distance *= 2
    else:
        pool = lax.psum(energy, "stripe")
    scores = energy / (pool / (stripes * stripes_here) + epsilon)
    return (
        syndrome.reshape(layers_here, stripes_here, PARITY, planes, byte_count),
        jnp.transpose(scores, (2, 0, 1)),
    )


def solution(mesh):
    return jax.shard_map(
        scrub,
        mesh=mesh,
        in_specs=(P("stripe", "node", None, None, None), P(), P()),
        out_specs=(P("node", "stripe", None, None, None), P("node", "stripe", None)),
        check_vma=False,
    )
```

```python
import jax
import jax.numpy as jnp
from jax import lax
from jax.experimental import pallas as pl
from jax.experimental.pallas import tpu as pltpu
from jax.sharding import PartitionSpec as P


PLANES = 8
PARITY = 4
DATA_NODES = 12
VIRTUAL = 2
OUT_ROWS = PARITY * PLANES
PARTS = 3


precise = lax.Precision.HIGHEST
epsilon = 1e-06
WIDTH = PARTS * 4 * PLANES
MIB = 1024 * 1024


def dot32(a, b):
    return jnp.dot(a, b, precision=precise)


def inverse_of(matrix):
    size = matrix.shape[0]
    row_ids = lax.broadcasted_iota(jnp.int32, (size, size), 0)
    left = matrix
    right = (row_ids == lax.broadcasted_iota(jnp.int32, (size, size), 1)).astype(jnp.float32)
    for at in range(size):
        scale = 1.0 / left[at : at + 1, at : at + 1]
        left_row = left[at : at + 1] * scale
        right_row = right[at : at + 1] * scale
        factor = left[:, at : at + 1]
        here = row_ids == at
        left = jnp.where(here, left_row, left - factor * left_row)
        right = jnp.where(here, right_row, right - factor * right_row)
    return 0.5 * (right + right.T)


def table_kernel(nodes_here, gamma_ref, coeffs_ref, lines_ref, extra_ref):
    column, _ = where_am_i(nodes_here)
    gamma = gamma_ref[...]
    gamma_t = gamma.T
    encode = encode_rows(coeffs_ref[...])
    eye_rows = lax.broadcasted_iota(jnp.int32, (PLANES, PLANES), 0)
    eye_lanes = lax.broadcasted_iota(jnp.int32, (PLANES, PLANES), 1)
    identity = (eye_rows == eye_lanes).astype(jnp.float32)
    inverse = inverse_of(identity + dot32(gamma_t, gamma))
    gain = dot32(gamma, inverse)
    wide_rows = lax.broadcasted_iota(jnp.int32, (PLANES, WIDTH), 0)
    wide_lanes = lax.broadcasted_iota(jnp.int32, (PLANES, WIDTH), 1)
    spread = (wide_rows == wide_lanes % PLANES).astype(jnp.float32)

    def tiled(matrix):
        return jnp.concatenate([dot32(matrix, spread)] * 4, axis=0)

    plain = jnp.concatenate([spread] * 4, axis=0)
    lower = tiled(identity - dot32(gain, gamma_t))
    upper = tiled(inverse)
    from_upper = tiled(-gain)
    from_lower = tiled(dot32(inverse, gamma_t))
    block_in = lax.broadcasted_iota(jnp.int32, (4 * PLANES, WIDTH), 0) // PLANES
    lanes = lax.broadcasted_iota(jnp.int32, (4 * PLANES, WIDTH), 1)
    block_out = (lanes // PLANES) % 4
    zero = jnp.zeros((4 * PLANES, WIDTH), jnp.float32)

    def parts(product):
        part = lax.broadcasted_iota(jnp.int32, product.shape, 1) // (4 * PLANES)
        head = product.astype(jnp.bfloat16).astype(jnp.float32)
        rest = product - head
        middle = rest.astype(jnp.bfloat16).astype(jnp.float32)
        tail = rest - middle
        chosen = jnp.where(part == 0, head, jnp.where(part == 1, middle, tail))
        return chosen.astype(jnp.bfloat16)

    def real(source, row):
        node = 4 * source + row
        return jnp.where((node < DATA_NODES - VIRTUAL) | (node >= DATA_NODES), 1.0, 0.0)

    upto3 = jnp.concatenate(encode[:3], axis=0)
    for o in range(4):
        source = column ^ o

        def own(digit):
            return jnp.where(source == digit, plain, jnp.where(source < digit, lower, upper))

        coupled = jnp.where(block_out < source, from_upper, from_lower)
        coupled = jnp.where((block_in == block_out) & (block_in != source), coupled, zero)
        for j in range(4):
            from_own = (block_in == source) & (block_out == j)
            step = jnp.where(from_own, own(j), jnp.where(source == j, coupled, zero))
            product = dot32(upto3, step)
            for row in range(3):
                piece = product[row * OUT_ROWS : (row + 1) * OUT_ROWS] * real(source, row)
                lines_ref[row, o, j * OUT_ROWS : (j + 1) * OUT_ROWS] = parts(piece)
            piece = dot32(encode[3], jnp.where(from_own, own(column), zero))
            piece = piece * real(source, 3)
            lines_ref[3, o, j * OUT_ROWS : (j + 1) * OUT_ROWS] = parts(piece)
    away = jnp.where(block_in < column, from_upper, from_lower)
    away = jnp.where((block_in == (column ^ block_out)) & (block_out != 0), away, zero)
    extra_ref[...] = parts(dot32(encode[3], away) * real(column, 3))


def encode_rows(coeffs):
    nodes = coeffs.shape[-1]
    flat = coeffs.reshape(OUT_ROWS * PLANES, nodes)
    lanes = lax.broadcasted_iota(jnp.int32, (nodes, 4 * OUT_ROWS), 1)
    node = 4 * ((lanes // PLANES) % 4) + lanes // OUT_ROWS
    pick = lax.broadcasted_iota(jnp.int32, (nodes, 4 * OUT_ROWS), 0) == node
    picked = dot32(flat, pick.astype(jnp.float32)).reshape(OUT_ROWS, PLANES, 4 * OUT_ROWS)
    plane = lax.broadcasted_iota(jnp.int32, picked.shape, 1)
    lane = lax.broadcasted_iota(jnp.int32, picked.shape, 2)
    data = jnp.sum(jnp.where(plane == lane % PLANES, picked, 0.0), axis=1)
    out = lax.broadcasted_iota(jnp.int32, (OUT_ROWS, 4 * PLANES), 0)
    into = lax.broadcasted_iota(jnp.int32, (OUT_ROWS, 4 * PLANES), 1)
    rows = []
    for row in range(4):
        parity = (into // PLANES == 3) & (out == row * PLANES + into % PLANES)
        taken = data[:, row * OUT_ROWS : (row + 1) * OUT_ROWS]
        rows.append(jnp.where(parity, 1.0, -taken))
    return rows


def build_tables(nodes_here, gamma, coeffs):
    return kernel_call(
        lambda *refs: table_kernel(nodes_here, *refs),
        (
            jax.ShapeDtypeStruct((4, 4, 4 * OUT_ROWS, WIDTH), jnp.bfloat16),
            jax.ShapeDtypeStruct((OUT_ROWS, WIDTH), jnp.bfloat16),
        ),
        (gamma, jnp.transpose(coeffs, (0, 2, 3, 1))),
        1000,
        1,
    )


def where_am_i(nodes_here):
    peers = 4 // nodes_here
    device = lax.axis_index("node")
    return device // peers, device % peers


def gathered(slabs):
    block = jnp.concatenate(slabs, axis=0)
    return jnp.concatenate([block] * PARTS, axis=0)


def line_at(number, row):
    shift = 2 * jnp.minimum(row, 2)
    base = ((number >> shift) << (shift + 2)) | (number & ((1 << shift) - 1))
    return [base + (at << shift) for at in range(4)]


def mixed(matrix, slabs):
    return jnp.dot(matrix, gathered(slabs), preferred_element_type=jnp.float32)


def own_kernel(layers_here, own_ref, lines_ref, extra_ref, out_ref):
    nodes_here = own_ref.shape[1]
    column_layers = out_ref.shape[0]
    column, peer = where_am_i(nodes_here)
    flip = peer * layers_here
    for local in range(nodes_here):
        row = peer * nodes_here + local

        def body(number, carry):
            line = line_at(number, row)
            total = mixed(
                lines_ref[row, 0],
                [own_ref[0, local, column * column_layers + layer] for layer in line],
            )
            for at, layer in enumerate(line):
                value = total[at * OUT_ROWS : (at + 1) * OUT_ROWS]
                spot = layer ^ flip
                out_ref[spot] = value if local == 0 else out_ref[spot] + value
            return carry

        lax.fori_loop(0, column_layers // 4, body, 0, unroll=8)

    @pl.when((peer + 1) * nodes_here == 4)
    def _():
        def body(layer, carry):
            away = [
                own_ref[0, nodes_here - 1, (column ^ o) * column_layers + layer] for o in range(4)
            ]
            out_ref[layer ^ flip] += mixed(extra_ref[...], away)
            return carry

        lax.fori_loop(0, column_layers, body, 0, unroll=8)


def add_rows(layers_here, nodes_here, lines_ref, pieces, before_ref, total_ref):
    _, peer = where_am_i(nodes_here)
    flip = peer * layers_here
    for order, (local, sources) in enumerate(pieces.items()):
        row = peer * nodes_here + local

        def body(number, carry):
            line = line_at(number, row)
            total = None
            for offset, ref in sources:
                term = mixed(lines_ref[row, offset], [ref[0, 0, layer] for layer in line])
                total = term if total is None else total + term
            for at, layer in enumerate(line):
                spot = layer ^ flip
                start = before_ref[spot] if order == 0 else total_ref[spot]
                total_ref[spot] = start + total[at * OUT_ROWS : (at + 1) * OUT_ROWS]
            return carry

        lax.fori_loop(0, total_ref.shape[0] // 4, body, 0, unroll=8)


def across_kernel(layers_here, nodes_here, lines_ref, before_ref, *refs):
    far_refs, total_ref = refs[:-1], refs[-1]
    pieces = {at: [(3, ref)] for at, ref in enumerate(far_refs)}
    add_rows(layers_here, nodes_here, lines_ref, pieces, before_ref, total_ref)


def beside_kernel(layers_here, nodes_here, rows, lines_ref, before_ref, *refs):
    piece_refs, out_refs, total_ref = refs[: 2 * rows], refs[2 * rows : -1], refs[-1]
    pieces = {at: [(1, piece_refs[2 * at]), (2, piece_refs[2 * at + 1])] for at in range(rows)}
    add_rows(layers_here, nodes_here, lines_ref, pieces, before_ref, total_ref)
    for slot in reversed(range(len(out_refs))):

        def copy(at, carry):
            out_refs[slot][at] = total_ref[slot * layers_here + at]
            return carry

        lax.fori_loop(0, layers_here, copy, 0, unroll=8)


def join_kernel(nodes_here, sums_count, lines_ref, *refs):
    sum_refs, piece_refs, total_ref = refs[:sums_count], refs[sums_count:-1], refs[-1]
    _, peer = where_am_i(nodes_here)
    row = peer * nodes_here + nodes_here - 1

    def body(number, carry):
        line = line_at(number, jnp.int32(1))
        total = None
        for order, ref in enumerate(piece_refs):
            term = mixed(lines_ref[row, 1 + order % 2], [ref[0, 0, layer] for layer in line])
            total = term if total is None else total + term
        for at, layer in enumerate(line):
            value = sum(ref[layer] for ref in sum_refs)
            if total is not None:
                value = value + total[at * OUT_ROWS : (at + 1) * OUT_ROWS]
            total_ref[layer] = value
        return carry

    lax.fori_loop(0, total_ref.shape[0] // 4, body, 0, unroll=8)


def finish_kernel(nodes_here, first, lines_ref, before_ref, *refs):
    earlier = 1 if first else 0
    piece_refs, refs = refs[: len(refs) - 3 - earlier], refs[len(refs) - 3 - earlier :]
    value_ref, energy_ref, lanes_ref = refs[earlier:]
    count, _, byte_count = value_ref.shape
    _, peer = where_am_i(nodes_here)
    for base in range(0, count, 16):
        for number in range(4):
            line = [base + number + 4 * at for at in range(4)]
            total = None
            for order, ref in enumerate(piece_refs):
                row = (peer ^ (1 + order // 2)) * nodes_here + nodes_here - 1
                term = mixed(lines_ref[row, 1 + order % 2], [ref[0, 0, layer] for layer in line])
                total = term if total is None else total + term
            for at, layer in enumerate(line):
                value = before_ref[first + layer]
                if total is not None:
                    value = value + total[at * OUT_ROWS : (at + 1) * OUT_ROWS]
                value_ref[layer] = value
                square = value * value
                lanes = sum(square[:, i * 128 : (i + 1) * 128] for i in range(byte_count // 128))
                for i in range(PARITY):
                    lanes_ref[i, layer : layer + 1] = jnp.sum(
                        lanes[i * PLANES : (i + 1) * PLANES], axis=0, keepdims=True
                    )
    lanes = jnp.concatenate([lanes_ref[i] for i in range(PARITY)], axis=0)
    energy = jnp.sum(lanes.T, axis=0, keepdims=True) * (1.0 / (PLANES * byte_count))
    if first:
        energy_ref[0, :, 0:first] = refs[0][0]
    for i in range(PARITY):
        energy_ref[0, i : i + 1, first : first + count] = energy[:, i * count : (i + 1) * count]


def store_kernel(first, value_ref, *refs):
    out_ref, sem = refs[-2:]
    rows = pl.ds(first, value_ref.shape[0])
    copy = pltpu.make_async_copy(value_ref, out_ref.at[rows], sem)
    copy.start()
    copy.wait()


def kernel_call(
    body, out_shape, operands, mflops, mib, in_specs=None, out_specs=None, scratch=(), vmem=16, aliases=None
):
    whole = pl.BlockSpec(memory_space=pltpu.VMEM)
    if out_specs is None:
        out_specs = jax.tree.map(lambda _: whole, out_shape)
    return pl.pallas_call(
        body,
        out_shape=out_shape,
        in_specs=in_specs or [whole] * len(operands),
        out_specs=out_specs,
        scratch_shapes=scratch,
        input_output_aliases=aliases or {},
        compiler_params=pltpu.CompilerParams(vmem_limit_bytes=vmem * MIB),
        cost_estimate=pl.CostEstimate(
            flops=mflops * 1_000_000, bytes_accessed=mib * MIB, transcendentals=0
        ),
    )(*operands)


def scrub(groups, gamma, coeffs):
    stripes_here, nodes_here, layers, planes, byte_count = groups.shape
    devices = lax.axis_size("node")
    peers = devices // 4
    layers_here = layers // devices
    column_layers = layers // 4
    direct = nodes_here == 2
    rows = nodes_here - 1 if direct else nodes_here

    halves = 2 if direct else 1
    half = layers_here // halves

    def cut(source, plan):
        def body(source_ref, *refs):
            column, peer = where_am_i(nodes_here)
            out_refs, sems = refs[:-1], refs[-1]
            copies = []
            for at, (row, offset, slot, start, count) in enumerate(plan):
                first = (column ^ offset) * column_layers + start
                if slot is not None:
                    first += (peer ^ slot) * layers_here
                piece = source_ref.at[:, pl.ds(row, 1), pl.ds(first, count)]
                copies.append(pltpu.make_async_copy(piece, out_refs[at], sems.at[at]))
                copies[-1].start()
            for copy in copies:
                copy.wait()

        shapes = [
            (stripes_here, 1, count, planes, byte_count) for _, _, _, _, count in plan
        ]
        return kernel_call(
            body,
            [jax.ShapeDtypeStruct(shape, groups.dtype) for shape in shapes],
            (source,),
            1,
            3,
            in_specs=[pl.BlockSpec(memory_space=pltpu.HBM)],
            scratch=[pltpu.SemaphoreType.DMA((len(plan),))],
            vmem=16,
        )

    def send(piece, offset, slot=0):
        route = [(i, (((i // peers) ^ offset) * peers + i % peers) ^ slot) for i in range(devices)]
        return lax.ppermute(piece, "node", route)

    column = lax.axis_index("node") // peers
    across_piece = lax.dynamic_slice(
        groups,
        (0, 0, (column ^ 3) * column_layers, 0, 0),
        (stripes_here, 1, column_layers, planes, byte_count),
    )
    source, across_piece = lax.optimization_barrier((groups, across_piece))
    across_piece = send(across_piece, 3)
    plan = [(at, 3, None, 0, column_layers) for at in range(1, nodes_here)]
    plan += [(at, offset, None, 0, column_layers) for at in range(rows) for offset in (1, 2)]
    if direct:
        for slot in range(peers):
            for start in range(0, layers_here, layers_here if slot == 0 else half):
                count = layers_here if slot == 0 else half
                plan += [(rows, offset, slot, start, count) for offset in (1, 2)]
    cuts = cut(source, plan)
    cuts = lax.optimization_barrier(tuple(cuts))
    arrived = [send(piece, entry[1], entry[2] or 0) for piece, entry in zip(cuts, plan)]
    across_pieces = [across_piece] + arrived[: nodes_here - 1]
    arrived = arrived[nodes_here - 1 :]
    beside_pieces, last_pieces = arrived[: 2 * rows], arrived[2 * rows :]
    lines, extra = build_tables(nodes_here, gamma, coeffs)

    all_layers = jax.ShapeDtypeStruct((column_layers, OUT_ROWS, byte_count), jnp.float32)
    part = jax.ShapeDtypeStruct((layers_here, OUT_ROWS, byte_count), jnp.float32)
    own = kernel_call(
        lambda *refs: own_kernel(layers_here, *refs), all_layers, (groups, lines, extra), 2000, 8
    )
    across = kernel_call(
        lambda *refs: across_kernel(layers_here, nodes_here, *refs),
        all_layers,
        (lines, own, *across_pieces),
        2000,
        9,
    )
    sums = kernel_call(
        lambda *refs: beside_kernel(layers_here, nodes_here, rows, *refs),
        [part] * peers,
        (lines, across, *beside_pieces),
        2000,
        9,
        scratch=[pltpu.VMEM(all_layers.shape, jnp.float32)],
    )
    parts = [sums[0]]
    for slot in range(1, peers):
        route = [(i, (i // peers) * peers + ((i % peers) ^ slot)) for i in range(devices)]
        parts.append(lax.ppermute(sums[slot], "node", route))
    total = kernel_call(
        lambda *refs: join_kernel(nodes_here, peers, *refs),
        part,
        (lines, *parts, *last_pieces[:2]),
        500,
        6,
    )

    any_space = pl.BlockSpec(memory_space=pl.ANY)
    whole = pl.BlockSpec(memory_space=pltpu.VMEM)
    syndrome, energy = [], []
    for at in range(halves):
        value, new_energy = kernel_call(
            lambda *refs: finish_kernel(nodes_here, at * half, *refs),
            (
                jax.ShapeDtypeStruct((half, OUT_ROWS, byte_count), jnp.float32),
                jax.ShapeDtypeStruct((stripes_here, PARITY, (at + 1) * half), jnp.float32),
            ),
            (lines, total, *last_pieces[2 + 2 * at :: 2 * halves], *last_pieces[3 + 2 * at :: 2 * halves], *energy),
            500,
            4,
            scratch=[pltpu.VMEM((PARITY, half, 128), jnp.float32)],
        )
        energy = [new_energy]
        syndrome = [
            kernel_call(
                lambda *refs: store_kernel(at * half, *refs),
                part,
                (value, *syndrome),
                1,
                4,
                in_specs=[whole] + [any_space] * at,
                out_specs=any_space,
                scratch=[pltpu.SemaphoreType.DMA(())],
                aliases={1: 0} if at else None,
            )
        ]
    (syndrome,), (energy,) = syndrome, energy
    stripes = lax.axis_size("stripe")
    pool = energy
    if stripes & (stripes - 1) == 0:
        distance = 1
        while distance < stripes:
            pool = pool + lax.ppermute(pool, "stripe", [(i, i ^ distance) for i in range(stripes)])
            distance *= 2
    else:
        pool = lax.psum(energy, "stripe")
    scores = energy / (pool / (stripes * stripes_here) + epsilon)
    return (
        syndrome.reshape(layers_here, stripes_here, PARITY, planes, byte_count),
        jnp.transpose(scores, (2, 0, 1)),
    )


def solution(mesh):
    return jax.shard_map(
        scrub,
        mesh=mesh,
        in_specs=(P("stripe", "node", None, None, None), P(), P()),
        out_specs=(P("node", "stripe", None, None, None), P("node", "stripe", None)),
        check_vma=False,
    )
```

```python
import jax
import jax.numpy as jnp
from jax import lax
from jax.experimental import pallas as pl
from jax.experimental.pallas import tpu as pltpu
from jax.sharding import PartitionSpec as P


PLANES = 8
PARITY = 4
DATA_NODES = 12
VIRTUAL = 2
OUT_ROWS = PARITY * PLANES
PARTS = 3


precise = lax.Precision.HIGHEST
epsilon = 1e-06
WIDTH = PARTS * 4 * PLANES
MIB = 1024 * 1024


def dot32(a, b):
    return jnp.dot(a, b, precision=precise)


def inverse_of(matrix):
    size = matrix.shape[0]
    row_ids = lax.broadcasted_iota(jnp.int32, (size, size), 0)
    left = matrix
    right = (row_ids == lax.broadcasted_iota(jnp.int32, (size, size), 1)).astype(jnp.float32)
    for at in range(size):
        scale = 1.0 / left[at : at + 1, at : at + 1]
        left_row = left[at : at + 1] * scale
        right_row = right[at : at + 1] * scale
        factor = left[:, at : at + 1]
        here = row_ids == at
        left = jnp.where(here, left_row, left - factor * left_row)
        right = jnp.where(here, right_row, right - factor * right_row)
    return 0.5 * (right + right.T)


def table_kernel(nodes_here, gamma_ref, coeffs_ref, lines_ref, extra_ref):
    column, _ = where_am_i(nodes_here)
    gamma = gamma_ref[...]
    gamma_t = gamma.T
    encode = encode_rows(coeffs_ref[...])
    eye_rows = lax.broadcasted_iota(jnp.int32, (PLANES, PLANES), 0)
    eye_lanes = lax.broadcasted_iota(jnp.int32, (PLANES, PLANES), 1)
    identity = (eye_rows == eye_lanes).astype(jnp.float32)
    inverse = inverse_of(identity + dot32(gamma_t, gamma))
    gain = dot32(gamma, inverse)
    wide_rows = lax.broadcasted_iota(jnp.int32, (PLANES, WIDTH), 0)
    wide_lanes = lax.broadcasted_iota(jnp.int32, (PLANES, WIDTH), 1)
    spread = (wide_rows == wide_lanes % PLANES).astype(jnp.float32)

    def tiled(matrix):
        return jnp.concatenate([dot32(matrix, spread)] * 4, axis=0)

    plain = jnp.concatenate([spread] * 4, axis=0)
    lower = tiled(identity - dot32(gain, gamma_t))
    upper = tiled(inverse)
    from_upper = tiled(-gain)
    from_lower = tiled(dot32(inverse, gamma_t))
    block_in = lax.broadcasted_iota(jnp.int32, (4 * PLANES, WIDTH), 0) // PLANES
    lanes = lax.broadcasted_iota(jnp.int32, (4 * PLANES, WIDTH), 1)
    block_out = (lanes // PLANES) % 4
    zero = jnp.zeros((4 * PLANES, WIDTH), jnp.float32)

    def parts(product):
        part = lax.broadcasted_iota(jnp.int32, product.shape, 1) // (4 * PLANES)
        head = product.astype(jnp.bfloat16).astype(jnp.float32)
        rest = product - head
        middle = rest.astype(jnp.bfloat16).astype(jnp.float32)
        tail = rest - middle
        chosen = jnp.where(part == 0, head, jnp.where(part == 1, middle, tail))
        return chosen.astype(jnp.bfloat16)

    def real(source, row):
        node = 4 * source + row
        return jnp.where((node < DATA_NODES - VIRTUAL) | (node >= DATA_NODES), 1.0, 0.0)

    upto3 = jnp.concatenate(encode[:3], axis=0)
    for o in range(4):
        source = column ^ o

        def own(digit):
            return jnp.where(source == digit, plain, jnp.where(source < digit, lower, upper))

        coupled = jnp.where(block_out < source, from_upper, from_lower)
        coupled = jnp.where((block_in == block_out) & (block_in != source), coupled, zero)
        for j in range(4):
            from_own = (block_in == source) & (block_out == j)
            step = jnp.where(from_own, own(j), jnp.where(source == j, coupled, zero))
            product = dot32(upto3, step)
            for row in range(3):
                piece = product[row * OUT_ROWS : (row + 1) * OUT_ROWS] * real(source, row)
                lines_ref[row, o, j * OUT_ROWS : (j + 1) * OUT_ROWS] = parts(piece)
            piece = dot32(encode[3], jnp.where(from_own, own(column), zero))
            piece = piece * real(source, 3)
            lines_ref[3, o, j * OUT_ROWS : (j + 1) * OUT_ROWS] = parts(piece)
    away = jnp.where(block_in < column, from_upper, from_lower)
    away = jnp.where((block_in == (column ^ block_out)) & (block_out != 0), away, zero)
    extra_ref[...] = parts(dot32(encode[3], away) * real(column, 3))


def encode_rows(coeffs):
    nodes = coeffs.shape[-1]
    flat = coeffs.reshape(OUT_ROWS * PLANES, nodes)
    lanes = lax.broadcasted_iota(jnp.int32, (nodes, 4 * OUT_ROWS), 1)
    node = 4 * ((lanes // PLANES) % 4) + lanes // OUT_ROWS
    pick = lax.broadcasted_iota(jnp.int32, (nodes, 4 * OUT_ROWS), 0) == node
    picked = dot32(flat, pick.astype(jnp.float32)).reshape(OUT_ROWS, PLANES, 4 * OUT_ROWS)
    plane = lax.broadcasted_iota(jnp.int32, picked.shape, 1)
    lane = lax.broadcasted_iota(jnp.int32, picked.shape, 2)
    data = jnp.sum(jnp.where(plane == lane % PLANES, picked, 0.0), axis=1)
    out = lax.broadcasted_iota(jnp.int32, (OUT_ROWS, 4 * PLANES), 0)
    into = lax.broadcasted_iota(jnp.int32, (OUT_ROWS, 4 * PLANES), 1)
    rows = []
    for row in range(4):
        parity = (into // PLANES == 3) & (out == row * PLANES + into % PLANES)
        taken = data[:, row * OUT_ROWS : (row + 1) * OUT_ROWS]
        rows.append(jnp.where(parity, 1.0, -taken))
    return rows


def build_tables(nodes_here, gamma, coeffs):
    return kernel_call(
        lambda *refs: table_kernel(nodes_here, *refs),
        (
            jax.ShapeDtypeStruct((4, 4, 4 * OUT_ROWS, WIDTH), jnp.bfloat16),
            jax.ShapeDtypeStruct((OUT_ROWS, WIDTH), jnp.bfloat16),
        ),
        (gamma, jnp.transpose(coeffs, (0, 2, 3, 1))),
        1000,
        1,
    )


def where_am_i(nodes_here):
    peers = 4 // nodes_here
    device = lax.axis_index("node")
    return device // peers, device % peers


def gathered(slabs):
    block = jnp.concatenate(slabs, axis=0)
    return jnp.concatenate([block] * PARTS, axis=0)


def line_at(number, row):
    shift = 2 * jnp.minimum(row, 2)
    base = ((number >> shift) << (shift + 2)) | (number & ((1 << shift) - 1))
    return [base + (at << shift) for at in range(4)]


def mixed(matrix, slabs):
    return jnp.dot(matrix, gathered(slabs), preferred_element_type=jnp.float32)


def own_kernel(layers_here, own_ref, lines_ref, extra_ref, out_ref):
    nodes_here = own_ref.shape[1]
    column_layers = out_ref.shape[0]
    column, peer = where_am_i(nodes_here)
    flip = peer * layers_here
    for local in range(nodes_here):
        row = peer * nodes_here + local

        def body(number, carry):
            line = line_at(number, row)
            total = mixed(
                lines_ref[row, 0],
                [own_ref[0, local, column * column_layers + layer] for layer in line],
            )
            for at, layer in enumerate(line):
                value = total[at * OUT_ROWS : (at + 1) * OUT_ROWS]
                spot = layer ^ flip
                out_ref[spot] = value if local == 0 else out_ref[spot] + value
            return carry

        lax.fori_loop(0, column_layers // 4, body, 0, unroll=8)

    @pl.when((peer + 1) * nodes_here == 4)
    def _():
        def body(layer, carry):
            away = [
                own_ref[0, nodes_here - 1, (column ^ o) * column_layers + layer] for o in range(4)
            ]
            out_ref[layer ^ flip] += mixed(extra_ref[...], away)
            return carry

        lax.fori_loop(0, column_layers, body, 0, unroll=8)


def add_rows(layers_here, nodes_here, lines_ref, pieces, before_ref, total_ref):
    _, peer = where_am_i(nodes_here)
    flip = peer * layers_here
    for order, (local, sources) in enumerate(pieces.items()):
        row = peer * nodes_here + local

        def body(number, carry):
            line = line_at(number, row)
            total = None
            for offset, ref in sources:
                term = mixed(lines_ref[row, offset], [ref[0, 0, layer] for layer in line])
                total = term if total is None else total + term
            for at, layer in enumerate(line):
                spot = layer ^ flip
                start = before_ref[spot] if order == 0 else total_ref[spot]
                total_ref[spot] = start + total[at * OUT_ROWS : (at + 1) * OUT_ROWS]
            return carry

        lax.fori_loop(0, total_ref.shape[0] // 4, body, 0, unroll=8)


def across_kernel(layers_here, nodes_here, lines_ref, before_ref, *refs):
    far_refs, total_ref = refs[:-1], refs[-1]
    pieces = {at: [(3, ref)] for at, ref in enumerate(far_refs)}
    add_rows(layers_here, nodes_here, lines_ref, pieces, before_ref, total_ref)


def beside_kernel(layers_here, nodes_here, rows, lines_ref, before_ref, *refs):
    piece_refs, out_refs, total_ref = refs[: 2 * rows], refs[2 * rows : -1], refs[-1]
    pieces = {at: [(2, piece_refs[2 * at]), (1, piece_refs[2 * at + 1])] for at in range(rows)}
    add_rows(layers_here, nodes_here, lines_ref, pieces, before_ref, total_ref)
    for slot in reversed(range(len(out_refs))):

        def copy(at, carry):
            out_refs[slot][at] = total_ref[slot * layers_here + at]
            return carry

        lax.fori_loop(0, layers_here, copy, 0, unroll=8)


def join_kernel(nodes_here, sums_count, lines_ref, *refs):
    sum_refs, piece_refs, total_ref = refs[:sums_count], refs[sums_count:-1], refs[-1]
    _, peer = where_am_i(nodes_here)
    row = peer * nodes_here + nodes_here - 1

    def body(number, carry):
        line = line_at(number, jnp.int32(1))
        total = None
        for order, ref in enumerate(piece_refs):
            term = mixed(lines_ref[row, 2 - order % 2], [ref[0, 0, layer] for layer in line])
            total = term if total is None else total + term
        for at, layer in enumerate(line):
            value = sum(ref[layer] for ref in sum_refs)
            if total is not None:
                value = value + total[at * OUT_ROWS : (at + 1) * OUT_ROWS]
            total_ref[layer] = value
        return carry

    lax.fori_loop(0, total_ref.shape[0] // 4, body, 0, unroll=8)


def finish_kernel(nodes_here, first, lines_ref, before_ref, *refs):
    earlier = 1 if first else 0
    piece_refs, refs = refs[: len(refs) - 3 - earlier], refs[len(refs) - 3 - earlier :]
    value_ref, energy_ref, lanes_ref = refs[earlier:]
    count, _, byte_count = value_ref.shape
    _, peer = where_am_i(nodes_here)
    for base in range(0, count, 16):
        for number in range(4):
            line = [base + number + 4 * at for at in range(4)]
            total = None
            for order, ref in enumerate(piece_refs):
                row = (peer ^ (1 + order // 2)) * nodes_here + nodes_here - 1
                term = mixed(lines_ref[row, 2 - order % 2], [ref[0, 0, layer] for layer in line])
                total = term if total is None else total + term
            for at, layer in enumerate(line):
                value = before_ref[first + layer]
                if total is not None:
                    value = value + total[at * OUT_ROWS : (at + 1) * OUT_ROWS]
                value_ref[layer] = value
                square = value * value
                lanes = sum(square[:, i * 128 : (i + 1) * 128] for i in range(byte_count // 128))
                for i in range(PARITY):
                    lanes_ref[i, layer : layer + 1] = jnp.sum(
                        lanes[i * PLANES : (i + 1) * PLANES], axis=0, keepdims=True
                    )
    lanes = jnp.concatenate([lanes_ref[i] for i in range(PARITY)], axis=0)
    energy = jnp.sum(lanes.T, axis=0, keepdims=True) * (1.0 / (PLANES * byte_count))
    if first:
        energy_ref[0, :, 0:first] = refs[0][0]
    for i in range(PARITY):
        energy_ref[0, i : i + 1, first : first + count] = energy[:, i * count : (i + 1) * count]


def store_kernel(first, value_ref, *refs):
    out_ref, sem = refs[-2:]
    rows = pl.ds(first, value_ref.shape[0])
    copy = pltpu.make_async_copy(value_ref, out_ref.at[rows], sem)
    copy.start()
    copy.wait()


def kernel_call(
    body, out_shape, operands, mflops, mib, in_specs=None, out_specs=None, scratch=(), vmem=16, aliases=None
):
    whole = pl.BlockSpec(memory_space=pltpu.VMEM)
    if out_specs is None:
        out_specs = jax.tree.map(lambda _: whole, out_shape)
    return pl.pallas_call(
        body,
        out_shape=out_shape,
        in_specs=in_specs or [whole] * len(operands),
        out_specs=out_specs,
        scratch_shapes=scratch,
        input_output_aliases=aliases or {},
        compiler_params=pltpu.CompilerParams(vmem_limit_bytes=vmem * MIB),
        cost_estimate=pl.CostEstimate(
            flops=mflops * 1_000_000, bytes_accessed=mib * MIB, transcendentals=0
        ),
    )(*operands)


def scrub(groups, gamma, coeffs):
    stripes_here, nodes_here, layers, planes, byte_count = groups.shape
    devices = lax.axis_size("node")
    peers = devices // 4
    layers_here = layers // devices
    column_layers = layers // 4
    direct = nodes_here == 2
    rows = nodes_here - 1 if direct else nodes_here

    halves = 2 if direct else 1
    half = layers_here // halves

    def cut(source, plan):
        def body(source_ref, *refs):
            column, peer = where_am_i(nodes_here)
            out_refs, sems = refs[:-1], refs[-1]
            copies = []
            for at, (row, offset, slot, start, count) in enumerate(plan):
                first = (column ^ offset) * column_layers + start
                if slot is not None:
                    first += (peer ^ slot) * layers_here
                piece = source_ref.at[:, pl.ds(row, 1), pl.ds(first, count)]
                copies.append(pltpu.make_async_copy(piece, out_refs[at], sems.at[at]))
                copies[-1].start()
            for copy in copies:
                copy.wait()

        shapes = [
            (stripes_here, 1, count, planes, byte_count) for _, _, _, _, count in plan
        ]
        return kernel_call(
            body,
            [jax.ShapeDtypeStruct(shape, groups.dtype) for shape in shapes],
            (source,),
            1,
            3,
            in_specs=[pl.BlockSpec(memory_space=pltpu.HBM)],
            scratch=[pltpu.SemaphoreType.DMA((len(plan),))],
            vmem=16,
        )

    def send(piece, offset, slot=0):
        route = [(i, (((i // peers) ^ offset) * peers + i % peers) ^ slot) for i in range(devices)]
        return lax.ppermute(piece, "node", route)

    column = lax.axis_index("node") // peers
    across_piece = lax.dynamic_slice(
        groups,
        (0, 0, (column ^ 3) * column_layers, 0, 0),
        (stripes_here, 1, column_layers, planes, byte_count),
    )
    source, across_piece = lax.optimization_barrier((groups, across_piece))
    across_piece = send(across_piece, 3)
    plan = [(at, 3, None, 0, column_layers) for at in range(1, nodes_here)]
    plan += [(at, offset, None, 0, column_layers) for at in range(rows) for offset in (2, 1)]
    if direct:
        for slot in range(peers):
            for start in range(0, layers_here, layers_here if slot == 0 else half):
                count = layers_here if slot == 0 else half
                plan += [(rows, offset, slot, start, count) for offset in (2, 1)]
    cuts = cut(source, plan)
    cuts = lax.optimization_barrier(tuple(cuts))
    arrived = [send(piece, entry[1], entry[2] or 0) for piece, entry in zip(cuts, plan)]
    across_pieces = [across_piece] + arrived[: nodes_here - 1]
    arrived = arrived[nodes_here - 1 :]
    beside_pieces, last_pieces = arrived[: 2 * rows], arrived[2 * rows :]
    lines, extra = build_tables(nodes_here, gamma, coeffs)

    all_layers = jax.ShapeDtypeStruct((column_layers, OUT_ROWS, byte_count), jnp.float32)
    part = jax.ShapeDtypeStruct((layers_here, OUT_ROWS, byte_count), jnp.float32)
    own = kernel_call(
        lambda *refs: own_kernel(layers_here, *refs), all_layers, (groups, lines, extra), 2000, 8
    )
    across = kernel_call(
        lambda *refs: across_kernel(layers_here, nodes_here, *refs),
        all_layers,
        (lines, own, *across_pieces),
        2000,
        9,
    )
    sums = kernel_call(
        lambda *refs: beside_kernel(layers_here, nodes_here, rows, *refs),
        [part] * peers,
        (lines, across, *beside_pieces),
        2000,
        9,
        scratch=[pltpu.VMEM(all_layers.shape, jnp.float32)],
    )
    parts = [sums[0]]
    for slot in range(1, peers):
        route = [(i, (i // peers) * peers + ((i % peers) ^ slot)) for i in range(devices)]
        parts.append(lax.ppermute(sums[slot], "node", route))
    total = kernel_call(
        lambda *refs: join_kernel(nodes_here, peers, *refs),
        part,
        (lines, *parts, *last_pieces[:2]),
        500,
        6,
    )

    any_space = pl.BlockSpec(memory_space=pl.ANY)
    whole = pl.BlockSpec(memory_space=pltpu.VMEM)
    syndrome, energy = [], []
    for at in range(halves):
        value, new_energy = kernel_call(
            lambda *refs: finish_kernel(nodes_here, at * half, *refs),
            (
                jax.ShapeDtypeStruct((half, OUT_ROWS, byte_count), jnp.float32),
                jax.ShapeDtypeStruct((stripes_here, PARITY, (at + 1) * half), jnp.float32),
            ),
            (lines, total, *last_pieces[2 + 2 * at :: 2 * halves], *last_pieces[3 + 2 * at :: 2 * halves], *energy),
            500,
            4,
            scratch=[pltpu.VMEM((PARITY, half, 128), jnp.float32)],
        )
        energy = [new_energy]
        syndrome = [
            kernel_call(
                lambda *refs: store_kernel(at * half, *refs),
                part,
                (value, *syndrome),
                1,
                4,
                in_specs=[whole] + [any_space] * at,
                out_specs=any_space,
                scratch=[pltpu.SemaphoreType.DMA(())],
                aliases={1: 0} if at else None,
            )
        ]
    (syndrome,), (energy,) = syndrome, energy
    stripes = lax.axis_size("stripe")
    pool = energy
    if stripes & (stripes - 1) == 0:
        distance = 1
        while distance < stripes:
            pool = pool + lax.ppermute(pool, "stripe", [(i, i ^ distance) for i in range(stripes)])
            distance *= 2
    else:
        pool = lax.psum(energy, "stripe")
    scores = energy / (pool / (stripes * stripes_here) + epsilon)
    return (
        syndrome.reshape(layers_here, stripes_here, PARITY, planes, byte_count),
        jnp.transpose(scores, (2, 0, 1)),
    )


def solution(mesh):
    return jax.shard_map(
        scrub,
        mesh=mesh,
        in_specs=(P("stripe", "node", None, None, None), P(), P()),
        out_specs=(P("node", "stripe", None, None, None), P("node", "stripe", None)),
        check_vma=False,
    )
```
